32 devices in a mesh: gz: 4 (over z), gy: 2 (over y), gx: 4 (over x, core).
Axes of the slice: x: 2, y: 2, z: 4, core: 2. Of those that a mesh axis runs over, the one named last changes fastest.
Arguments:
- nz_vals: float32 [2097152], P(('gz', 'gy', 'gx'))
- idx_i: int32 [2097152], P(('gz', 'gy', 'gx'))
- idx_j: int32 [2097152], P(('gz', 'gy', 'gx'))
- idx_k: int32 [2097152], P(('gz', 'gy', 'gx'))
- fac_a: float32 [301056, 64], P(('gx', 'gz', 'gy'))
- fac_b: float32 [110592, 64], P(('gy', 'gz', 'gx'))
- fac_c: float32 [112640, 64], P(('gz', 'gy', 'gx'))
Outputs:
- output 1: float32 [301056, 64], P(('gx', 'gz', 'gy'))
- output 2: float32 [110592, 64], P(('gy', 'gz', 'gx'))
- output 3: float32 [112640, 64], P(('gz', 'gy', 'gx'))
- output 4: float32 [64], replicated
All inputs are finite; a program needn't handle non-finite values.
Results may differ from the reference program's by a relative error of at most 0.001.
Values are sent between devices in bfloat16 or wider.
A program may use at most 1 GiB of HBM per device.

```python
import jax
import jax.numpy as jnp
from jax import lax

DIM_I = 301056
DIM_J = 110592
DIM_K = 112640
RANK = 64
NNZ_DEV = 65536
GZ = 4
GY = 2
GX = 4

DEVS = GZ * GY * GX
SLAB_I = DIM_I // GX
SLAB_J = DIM_J // GY
SLAB_K = DIM_K // GZ
VAL_SCALE = float(DIM_I) * float(DIM_J) * float(DIM_K) / float(DEVS * NNZ_DEV)
PROX_WEIGHT = 0.5


def draw_rows(key, slab_rows, is_valid):
    key_pick, key_hub, key_any = jax.random.split(key, 3)
    any_rows = jax.random.randint(key_any, (DEVS, NNZ_DEV), 0, slab_rows)
    hub_rows = jax.random.randint(key_hub, (DEVS, NNZ_DEV), 0, max(1, slab_rows // 16))
    pick_hub = jax.random.randint(key_pick, (DEVS, NNZ_DEV), 0, 4)
    local_rows = jnp.where(pick_hub == 0, hub_rows, any_rows)
    return jnp.where(is_valid, local_rows, 0).astype(jnp.int32).reshape(-1)


def draw_factor(key, num_rows):
    key_row, key_blk = jax.random.split(key)
    base_rows = 1.0 + jax.random.normal(key_row, (DEVS, num_rows // DEVS, RANK), jnp.float32)
    blk_scale = jnp.exp(0.5 * jax.random.normal(key_blk, (DEVS, 1, 1), jnp.float32))
    return (base_rows * blk_scale).reshape(num_rows, RANK)


def setup_inputs(seed: int = 0) -> dict:
    keys = jax.random.split(jax.random.key(seed), 8)
    counts = jax.random.randint(keys[0], (DEVS,), NNZ_DEV // 4, NNZ_DEV + 1)
    counts = jnp.where(jnp.arange(DEVS) == 0, NNZ_DEV, counts)
    is_valid = jnp.arange(NNZ_DEV)[None, :] < counts[:, None]
    raw_vals = 0.5 + jax.random.uniform(keys[1], (DEVS, NNZ_DEV), jnp.float32)
    nz_vals = jnp.where(is_valid, raw_vals * VAL_SCALE, 0.0).astype(jnp.float32).reshape(-1)
    return {
        "nz_vals": nz_vals,
        "idx_i": draw_rows(keys[2], SLAB_I, is_valid),
        "idx_j": draw_rows(keys[3], SLAB_J, is_valid),
        "idx_k": draw_rows(keys[4], SLAB_K, is_valid),
        "fac_a": draw_factor(keys[5], DIM_I),
        "fac_b": draw_factor(keys[6], DIM_J),
        "fac_c": draw_factor(keys[7], DIM_K),
    }


def to_global(local_idx, slab_rows, grid_axis):
    nz_grid = local_idx.reshape(GZ, GY, GX, NNZ_DEV)
    offset = lax.broadcasted_iota(jnp.int32, (GZ, GY, GX, 1), grid_axis) * slab_rows
    return (nz_grid + offset).reshape(DEVS, NNZ_DEV)


def mode_product(val_grid, out_rows, rows_one, rows_two, fac_one, fac_two, num_rows):
    buf_one = fac_one.astype(jnp.bfloat16).astype(jnp.float32)
    buf_two = fac_two.astype(jnp.bfloat16).astype(jnp.float32)

    def add_block(acc_rows, block_in):
        val_blk, out_blk, one_blk, two_blk = block_in
        contrib = val_blk[:, None] * (buf_one[one_blk] * buf_two[two_blk])
        return acc_rows.at[out_blk].add(contrib), None

    acc_rows, _ = lax.scan(add_block, jnp.zeros((num_rows, RANK), jnp.float32), (val_grid, out_rows, rows_one, rows_two))
    return acc_rows


def gram_of(fac):
    return jnp.dot(fac.T, fac, preferred_element_type=jnp.float32)


def spd_inverse(sys_mat):
    mat_order = sys_mat.shape[0]
    row_ids = jnp.arange(mat_order)[:, None]
    augmented = jnp.concatenate([sys_mat, jnp.eye(mat_order, dtype=sys_mat.dtype)], axis=1)

    def elim_step(pivot_idx, aug_rows):
        pivot_row = lax.dynamic_slice_in_dim(aug_rows, pivot_idx, 1, axis=0)
        pivot_val = lax.dynamic_slice_in_dim(pivot_row, pivot_idx, 1, axis=1)
        pivot_row = pivot_row / pivot_val
        pivot_col = lax.dynamic_slice_in_dim(aug_rows, pivot_idx, 1, axis=1)
        return jnp.where(row_ids == pivot_idx, pivot_row, aug_rows - pivot_col * pivot_row)

    augmented = lax.fori_loop(0, mat_order, elim_step, augmented)
    return augmented[:, mat_order:]


def update_factor(m_rows, old_rows, gram_one, gram_two, num_rows):
    gram_mat = gram_one * gram_two
    prox_term = PROX_WEIGHT * jnp.trace(gram_mat) / RANK
    inv_gram = spd_inverse(gram_mat + prox_term * jnp.eye(RANK, dtype=jnp.float32))
    fresh_rows = jnp.dot(m_rows + prox_term * old_rows, inv_gram, preferred_element_type=jnp.float32)
    col_scale = jnp.sqrt(jnp.sum(fresh_rows * fresh_rows, axis=0) / num_rows)
    return fresh_rows / col_scale, col_scale


def reference(nz_vals, idx_i, idx_j, idx_k, fac_a, fac_b, fac_c):
    val_grid = nz_vals.reshape(DEVS, NNZ_DEV)
    rows_i = to_global(idx_i, SLAB_I, 2)
    rows_j = to_global(idx_j, SLAB_J, 1)
    rows_k = to_global(idx_k, SLAB_K, 0)
    gram_b = gram_of(fac_b)
    gram_c = gram_of(fac_c)
    m_a = mode_product(val_grid, rows_i, rows_j, rows_k, fac_b, fac_c, DIM_I)
    out_a, _ = update_factor(m_a, fac_a, gram_b, gram_c, DIM_I)
    gram_a = gram_of(out_a)
    m_b = mode_product(val_grid, rows_j, rows_i, rows_k, out_a, fac_c, DIM_J)
    out_b, _ = update_factor(m_b, fac_b, gram_a, gram_c, DIM_J)
    gram_nb = gram_of(out_b)
    m_c = mode_product(val_grid, rows_k, rows_i, rows_j, out_a, out_b, DIM_K)
    out_c, lambdas = update_factor(m_c, fac_c, gram_a, gram_nb, DIM_K)
    return (out_a, out_b, out_c, lambdas)
```

```python
import functools

import jax
import jax.numpy as jnp
from jax import lax
from jax.experimental import pallas as pl
from jax.experimental.pallas import tpu as pltpu
from jax.sharding import PartitionSpec as P

HIGHEST = lax.Precision.HIGHEST
PROX_WEIGHT = 0.5
ALL_AXES = ("gz", "gy", "gx")

LANES = 128
RANK = 64
BLOCK = 1024
UNROLL = 16
STEPS = LANES // UNROLL
CHUNK = 8192
VMEM_MAX = 67_000_000


def lines_of(own_rows):
    return pl.cdiv(own_rows, 256) * 128


def place_rows(idx, own_rows):
    blk = idx // own_rows
    q = idx - blk * own_rows
    line = blk * lines_of(own_rows) + ((q >> 8) << 7) + (q & 127)
    return line, (q >> 7) & 1


def _bit(n):
    return 1 << n if n < 31 else -(1 << 31)


def mttkrp_body(
    rows_out, rows_one, rows_two, chunk, stage_rows,
    nblk_ref, flag_ref, out_h, one_h, two_h, val_ref, code_ref, line_ref, tab1_h, tab2_h, sum_h,
    acc, acc2, tab1, tab2, stage, raw1a, raw1b, raw2a, raw2b, contrib_a, contrib_b,
    sm_out, sm_one, sm_two, sem_idx, sem_tab, sem_out,
):
    raw1, raw2, contrib = (raw1a, raw1b), (raw2a, raw2b), (contrib_a, contrib_b)
    nblk = nblk_ref[0]
    blk_chunk = chunk // BLOCK
    nchunk = lax.div(nblk + (blk_chunk - 1), blk_chunk)

    def idx_copies(c, slot):
        src = pl.ds(pl.multiple_of(c * chunk, chunk), chunk)
        dst = pl.ds(pl.multiple_of(slot * chunk, chunk), chunk)
        pairs = ((out_h, sm_out), (one_h, sm_one), (two_h, sm_two))
        return [pltpu.make_async_copy(h.at[src], s.at[dst], sem_idx.at[slot, n]) for n, (h, s) in enumerate(pairs)]

    for cp in idx_copies(0, 0):
        cp.start()

    def tab_copy(tab_h, i, slot):
        src = tab_h.at[pl.ds(pl.multiple_of(i * stage_rows, stage_rows), stage_rows), :]
        return pltpu.make_async_copy(src, stage.at[slot], sem_tab.at[slot])

    tab_copy(tab1_h, 0, 0).start()

    def zero(r, _):
        at = pl.ds(pl.multiple_of(r * 128, 128), 128)
        acc[at, :] = jnp.zeros((128, LANES), jnp.float32)
        acc2[at, :] = jnp.zeros((128, LANES), jnp.float32)
        return 0

    lax.fori_loop(0, rows_out // 128, zero, 0)
    acc[pl.ds(rows_out, 16), :] = jnp.zeros((16, LANES), jnp.float32)
    acc2[pl.ds(rows_out, 16), :] = jnp.zeros((16, LANES), jnp.float32)

    def widen_table(tab_h, tab, rows, first_started):
        n = rows // stage_rows
        if not first_started:
            tab_copy(tab_h, 0, 0).start()

        def step(i, _):
            slot = lax.rem(i, 2)

            @pl.when(i + 1 < n)
            def _():
                tab_copy(tab_h, i + 1, 1 - slot).start()

            tab_copy(tab_h, i, slot).wait()

            def widen(r, _):
                at = pl.multiple_of(r * 64, 64)
                dst = pl.ds(pl.multiple_of(i * stage_rows + at, 64), 64)
                tab[dst, :] = stage[slot, pl.ds(at, 64), :].astype(jnp.float32)
                return 0

            lax.fori_loop(0, stage_rows // 64, widen, 0)
            return 0

        lax.fori_loop(0, n, step, 0)

    widen_table(tab1_h, tab1, rows_one, True)
    widen_table(tab2_h, tab2, rows_two, False)

    sub = lax.broadcasted_iota(jnp.int32, (8, LANES), 0)
    lane_id = lax.broadcasted_iota(jnp.int32, (8, LANES), 1)
    right = lane_id >= RANK
    span = 2 * chunk - (7 * 128 + UNROLL - 1)

    def at(sm, s, t):
        return sm.at[pl.ds(128 * s + t, span)]

    def pick(block, lane):
        index = jnp.full((8, LANES), lane, jnp.int32)
        return jnp.take_along_axis(block, index, axis=1, mode="promise_in_bounds")

    def rows8(tab, sm, r, t):
        x = jnp.broadcast_to(tab[pl.ds(at(sm, 0, t)[r], 1), :], (8, LANES))
        for s in range(1, 8):
            row = jnp.broadcast_to(tab[pl.ds(at(sm, s, t)[r], 1), :], (8, LANES))
            x = jnp.where(sub == s, row, x)
        return x

    def gather_group(par, r, t):
        g = slice(8 * t, 8 * t + 8)
        raw1[par][g, :] = rows8(tab1, sm_one, r, t)
        raw2[par][g, :] = rows8(tab2, sm_two, r, t)

    def product_group(par, t, vals, turns, keeps, lane0):
        g = slice(8 * t, 8 * t + 8)
        val = pick(vals, lane0 + t)
        x1, x2 = raw1[par][g, :], raw2[par][g, :]
        x1 = jnp.where((turns & _bit(t)) != 0, pltpu.roll(x1, RANK, axis=1), x1)
        x2 = jnp.where((turns & _bit(16 + t)) != 0, pltpu.roll(x2, RANK, axis=1), x2)
        contrib[par][g, :] = jnp.where((keeps & _bit(t)) != 0, val * (x1 * x2), 0.0)

    def add_group(par, r, t):
        x = contrib[par][8 * t : 8 * t + 8, :]
        row = [at(sm_out, s, t)[r] for s in range(8)]
        dst = acc if t % 2 == 0 else acc2
        sums = [dst[pl.ds(row[s], 8), :] + x for s in range(8)]
        for s in range(8):
            pltpu.store(dst.at[pl.ds(row[s], 8), :], sums[s], mask=(sub == s))

    def merge(par, b, q, flag):
        lines = line_ref[pl.ds(pl.multiple_of(b * 8, 8), 8), :] + sub

        def one(t, _):
            @pl.when((lax.shift_right_logical(flag, t) & 1) == 1)
            def _():
                line = pick(lines, q * UNROLL + t)
                rows = pl.ds(pl.multiple_of(t * 8, 8), 8)
                y = contrib[par][rows, :]
                total = y
                for d in range(1, 8):
                    same = (line == pltpu.roll(line, d, axis=0)) & (sub >= d)
                    total = total + jnp.where(same, pltpu.roll(y, d, axis=0), 0.0)
                contrib[par][rows, :] = total

            return 0

        lax.fori_loop(0, UNROLL, one, 0)

    def chunk_step(c, _):
        slot = lax.rem(c, 2)
        for cp in idx_copies(c, slot):
            cp.wait()

        @pl.when(c + 1 < nchunk)
        def _():
            for cp in idx_copies(c + 1, 1 - slot):
                cp.start()

        n_it = jnp.minimum(blk_chunk, nblk - c * blk_chunk) * STEPS
        last = n_it - 1
        base = slot * chunk

        def place(k):
            bl = k // STEPS
            q = k - bl * STEPS
            return c * blk_chunk + bl, q, base + bl * BLOCK + q * UNROLL

        def block_of(ref, b):
            return ref[pl.ds(pl.multiple_of(b * 8, 8), 8), :]

        def front(k):
            b, q, _ = place(jnp.minimum(k, last))
            codes = block_of(code_ref, b)
            keeps = pick(codes, q + STEPS)
            return block_of(val_ref, b), pick(codes, q), jnp.where(right, keeps, ~keeps), q * UNROLL

        def fetch(par, k):
            _, _, r = place(jnp.minimum(k, last))
            for t in range(UNROLL):
                gather_group(par, r, t)

        fetch(0, 0)
        args0 = front(0)
        for t in range(UNROLL):
            product_group(0, t, *args0)
        fetch(1, 1)

        def step(j, _):
            for par in range(2):
                k = 2 * j + par
                b, q, r = place(k)
                flag = flag_ref[c * (blk_chunk * STEPS) + k]

                @pl.when(flag != 0)
                def _():
                    merge(par, b, q, flag)

                args = front(k + 1)
                _, _, rn = place(jnp.minimum(k + 2, last))
                for t in range(UNROLL):
                    add_group(par, r, t)
                    product_group(1 - par, t, *args)
                    gather_group(par, rn, t)
            return 0

        lax.fori_loop(0, lax.div(n_it, 2), step, 0)
        return 0

    lax.fori_loop(0, nchunk, chunk_step, 0)

    def total(r, _):
        rows = pl.ds(pl.multiple_of(r * 64 + 8, 8), 64)
        acc[rows, :] = acc[rows, :] + acc2[rows, :]
        return 0

    lax.fori_loop(0, rows_out // 64, total, 0)
    cp = pltpu.make_async_copy(acc.at[pl.ds(8, rows_out), :], sum_h, sem_out)
    cp.start()
    cp.wait()


def mttkrp(name, plan, tab1, tab2, rows_out):
    nblk, flags, line_out, line_one, line_two, vals, code = plan
    nnz = line_out.shape[0]
    rows_one, rows_two = tab1.shape[0], tab2.shape[0]
    chunk = min(CHUNK, nnz)
    stage_rows = 896 if rows_one % 896 == 0 and rows_two % 896 == 0 else 128
    smem = pl.BlockSpec(memory_space=pltpu.SMEM)
    anym = pl.BlockSpec(memory_space=pl.ANY)
    vmem = pl.BlockSpec(memory_space=pltpu.VMEM)
    tiles = (nnz // LANES, LANES)
    step_buf = pltpu.VMEM((8 * UNROLL, LANES), jnp.float32)
    return pl.pallas_call(
        functools.partial(mttkrp_body, rows_out, rows_one, rows_two, chunk, stage_rows),
        out_shape=jax.ShapeDtypeStruct((rows_out, LANES), jnp.float32),
        in_specs=[smem, smem, anym, anym, anym, vmem, vmem, vmem, anym, anym],
        out_specs=anym,
        scratch_shapes=[
            pltpu.VMEM((rows_out + 16, LANES), jnp.float32),
            pltpu.VMEM((rows_out + 16, LANES), jnp.float32),
            pltpu.VMEM((rows_one, LANES), jnp.float32),
            pltpu.VMEM((rows_two, LANES), jnp.float32),
            pltpu.VMEM((2, stage_rows, LANES), jnp.bfloat16),
            *([step_buf] * 6),
            pltpu.SMEM((2 * chunk,), jnp.int32),
            pltpu.SMEM((2 * chunk,), jnp.int32),
            pltpu.SMEM((2 * chunk,), jnp.int32),
            pltpu.SemaphoreType.DMA((2, 3)),
            pltpu.SemaphoreType.DMA((2,)),
            pltpu.SemaphoreType.DMA,
        ],
        name=name,
        compiler_params=pltpu.CompilerParams(vmem_limit_bytes=VMEM_MAX),
        cost_estimate=pl.CostEstimate(flops=2_000_000_000, bytes_accessed=50_000_000, transcendentals=0),
    )(nblk, flags, line_out, line_one, line_two, vals.reshape(tiles), code, line_out.reshape(tiles), tab1, tab2)


def plan_mode(nblk, nz_vals, out_place, one_place, two_place, rows_out):
    nnz = nz_vals.shape[0]
    shape = (nnz // BLOCK, 8, LANES)
    sub = lax.broadcasted_iota(jnp.int32, shape, 1)
    line = jnp.where(nz_vals != 0, out_place[0], rows_out).reshape(shape)
    repeated = jnp.zeros((shape[0], LANES), jnp.bool_)
    for d in range(1, 8):
        same = (line[:, d:] == line[:, : 8 - d]) & (line[:, d:] != rows_out)
        repeated = repeated | jnp.any(same, axis=1)
    lane = jnp.arange(LANES)
    powers = jnp.where(lane[:, None] // UNROLL == jnp.arange(STEPS)[None, :], 1 << (lane[:, None] % UNROLL), 0)

    def words(bits):
        out = jnp.dot(bits.astype(jnp.bfloat16), powers.astype(jnp.bfloat16), preferred_element_type=jnp.float32)
        return out.astype(jnp.int32)

    rows = (nnz // LANES, LANES)
    half = out_place[1].reshape(rows)
    turn_one = words(one_place[1].reshape(rows) ^ half)
    turn_two = words(two_place[1].reshape(rows) ^ half)
    pad = jnp.zeros((rows[0], LANES - 2 * STEPS), jnp.int32)
    code = jnp.concatenate([turn_one | (turn_two << 16), words(half), pad], axis=1)
    flags = words(repeated).reshape(-1)
    return nblk, flags, (line + 8 - sub).reshape(nnz), one_place[0], two_place[0], nz_vals, code


def dot_t(a, b, dims):
    return lax.dot_general(a, b, (dims, ((), ())), precision=HIGHEST, preferred_element_type=jnp.float32)


def col_tiles(width, body, tail):
    full = width // 256
    if full:
        lax.fori_loop(0, full, lambda t, _: (body(t), 0)[1], 0)
    if width % 256:
        tail(full, width % 256)


def pack_tile(x, out_ref, t):
    w = x.shape[1]
    if w < 256:
        x = jnp.concatenate([x, jnp.zeros((RANK, 256 - w), jnp.float32)], axis=1)
    both = jnp.concatenate([x[:, :128], x[:, 128:]], axis=0)
    at = t * 128 if isinstance(t, int) else pl.multiple_of(t * 128, 128)
    out_ref[pl.ds(at, 128), :] = both.T.astype(jnp.bfloat16)


def cols(ref, t, w):
    at = t * 256 if isinstance(t, int) else pl.multiple_of(t * 256, 256)
    return ref.at[:, pl.ds(at, w)]


def prep_body(b_ref, c_ref, pack_b, pack_c, gram_b, gram_c):
    for src, pack, gram in ((b_ref, pack_b, gram_b), (c_ref, pack_c, gram_c)):
        gram[...] = jnp.zeros((RANK, RANK), jnp.float32)

        def tile(t, w, src=src, pack=pack, gram=gram):
            x = cols(src, t, w)[...]
            pack_tile(x, pack, t)
            gram[...] += dot_t(x, x, ((1,), (1,)))

        col_tiles(src.shape[1], lambda t: tile(t, 256), tile)


def prep(fac_b_t, fac_c_t):
    packs = [jax.ShapeDtypeStruct((lines_of(f.shape[1]), LANES), jnp.bfloat16) for f in (fac_b_t, fac_c_t)]
    gram = jax.ShapeDtypeStruct((RANK, RANK), jnp.float32)
    return pl.pallas_call(prep_body, out_shape=(*packs, gram, gram), name="prep")(fac_b_t, fac_c_t)


def invert_body(g1_ref, g2_ref, inv_ref, mu_ref, aug):
    order = RANK
    gram = g1_ref[...] * g2_ref[...]
    row_id = lax.broadcasted_iota(jnp.int32, (order, order), 0)
    col_id = lax.broadcasted_iota(jnp.int32, (order, order), 1)
    diag = row_id == col_id
    mu = PROX_WEIGHT * jnp.sum(jnp.where(diag, gram, 0.0), keepdims=True) / order
    mu_ref[...] = jnp.broadcast_to(mu, (8, LANES))
    eye = jnp.where(diag, 1.0, 0.0)
    aug[...] = jnp.concatenate([gram + mu * eye, eye], axis=1)
    rows = lax.broadcasted_iota(jnp.int32, (order, 2 * order), 0)
    lanes = lax.broadcasted_iota(jnp.int32, (order, 2 * order), 1)

    def eliminate(p, _):
        full = aug[...]
        row = aug[pl.ds(p, 1), :]
        col = jnp.sum(jnp.where(lanes == p, full, 0.0), axis=1, keepdims=True)
        pivot = jnp.sum(jnp.where(lanes[:1] == p, row, 0.0), axis=1, keepdims=True)
        row = row / pivot
        aug[...] = jnp.where(rows == p, row, full - col * row)
        return 0

    lax.fori_loop(0, order, eliminate, 0)
    inv_ref[...] = aug[:, order:]


def invert(name, gram_one, gram_two):
    return pl.pallas_call(
        invert_body,
        out_shape=(jax.ShapeDtypeStruct((RANK, RANK), jnp.float32), jax.ShapeDtypeStruct((8, LANES), jnp.float32)),
        scratch_shapes=[pltpu.VMEM((RANK, 2 * RANK), jnp.float32)],
        name=name,
    )(gram_one, gram_two)


def solve_body(m_ref, old_ref, inv_ref, mu_ref, fresh_ref, gram_ref):
    gram_ref[...] = jnp.zeros((RANK, RANK), jnp.float32)
    inv = inv_ref[...]
    mu = mu_ref[:1, :1]

    def tile(t, w):
        at = t * 128 if isinstance(t, int) else pl.multiple_of(t * 128, 128)
        m = m_ref[pl.ds(at, 128), :].T
        m = jnp.concatenate([m[:RANK], m[RANK:]], axis=1)[:, :w]
        y = m + mu * cols(old_ref, t, w)[...]
        x = dot_t(inv, y, ((0,), (0,)))
        cols(fresh_ref, t, w)[...] = x
        gram_ref[...] += dot_t(x, x, ((1,), (1,)))

    col_tiles(old_ref.shape[1], lambda t: tile(t, 256), tile)


def solve(name, m_own, old_t, inv, mu):
    return pl.pallas_call(
        solve_body,
        out_shape=(jax.ShapeDtypeStruct(old_t.shape, jnp.float32), jax.ShapeDtypeStruct((RANK, RANK), jnp.float32)),
        name=name,
    )(m_own, old_t, inv, mu)


def scale_body(total_rows, want_pack, fresh_ref, gram_ref, out_ref, lam_ref, scaled_ref, *pack_ref):
    gram = gram_ref[...]
    row_id = lax.broadcasted_iota(jnp.int32, (RANK, RANK), 0)
    col_id = lax.broadcasted_iota(jnp.int32, (RANK, RANK), 1)
    square = jnp.where(row_id == col_id, gram, 0.0)
    lam_col = jnp.sqrt(jnp.sum(square, axis=1, keepdims=True) / total_rows)
    lam_row = jnp.sqrt(jnp.sum(square, axis=0, keepdims=True) / total_rows)
    lam_ref[...] = lam_row
    scaled_ref[...] = gram / lam_col / lam_row

    def tile(t, w):
        x = cols(fresh_ref, t, w)[...] / lam_col
        cols(out_ref, t, w)[...] = x
        if want_pack:
            pack_tile(x, pack_ref[0], t)

    col_tiles(fresh_ref.shape[1], lambda t: tile(t, 256), tile)


def scale(name, fresh_t, gram_sum, total_rows, want_pack):
    own = fresh_t.shape[1]
    outs = [
        jax.ShapeDtypeStruct(fresh_t.shape, jnp.float32),
        jax.ShapeDtypeStruct((1, RANK), jnp.float32),
        jax.ShapeDtypeStruct((RANK, RANK), jnp.float32),
    ]
    if want_pack:
        outs.append(jax.ShapeDtypeStruct((lines_of(own), LANES), jnp.bfloat16))
    return pl.pallas_call(functools.partial(scale_body, total_rows, want_pack), out_shape=tuple(outs), name=name)(fresh_t, gram_sum)


def expand_slab(own_lines, owner_axes):
    return lax.all_gather(own_lines, owner_axes, axis=0, tiled=True)


def fold_slab(part_lines, owner_axes):
    return lax.psum_scatter(part_lines, owner_axes, scatter_dimension=0, tiled=True)


def solution(mesh):
    size_z = mesh.shape["gz"]
    size_y = mesh.shape["gy"]
    size_x = mesh.shape["gx"]
    n_dev = size_z * size_y * size_x
    owners_a = ("gz", "gy")
    owners_b = ("gz", "gx")
    owners_c = ("gy", "gx")

    def device_step(nz_vals, idx_i, idx_j, idx_k, fac_a, fac_b, fac_c):
        own_a, own_b, own_c = fac_a.shape[0], fac_b.shape[0], fac_c.shape[0]
        rows_a = lines_of(own_a) * (n_dev // size_x)
        rows_b = lines_of(own_b) * (n_dev // size_y)
        rows_c = lines_of(own_c) * (n_dev // size_z)
        old_a, old_b, old_c = fac_a.T, fac_b.T, fac_c.T

        pack_b, pack_c, gram_b, gram_c = prep(old_b, old_c)
        gram_b, gram_c = lax.psum((gram_b, gram_c), ALL_AXES)
        buf_b = expand_slab(pack_b, owners_b)
        buf_c = expand_slab(pack_c, owners_c)

        at_a = place_rows(idx_i, own_a)
        at_b = place_rows(idx_j, own_b)
        at_c = place_rows(idx_k, own_c)
        used = jnp.max(jnp.where(nz_vals != 0, jnp.arange(nz_vals.shape[0], dtype=jnp.int32) + 1, 1))
        nblk = ((used + (BLOCK - 1)) // BLOCK).reshape(1)

        plan_a = plan_mode(nblk, nz_vals, at_a, at_b, at_c, rows_a)
        part_a = mttkrp("mttkrp_a", plan_a, buf_b, buf_c, rows_a)
        inv, mu = invert("invert_a", gram_b, gram_c)
        fresh, gram = solve("solve_a", fold_slab(part_a, owners_a), old_a, inv, mu)
        out_a, _, gram_a, pack_a = scale("scale_a", fresh, lax.psum(gram, ALL_AXES), own_a * n_dev, True)
        buf_a = expand_slab(pack_a, owners_a)

        plan_b = plan_mode(nblk, nz_vals, at_b, at_a, at_c, rows_b)
        part_b = mttkrp("mttkrp_b", plan_b, buf_a, buf_c, rows_b)
        inv, mu = invert("invert_b", gram_a, gram_c)
        fresh, gram = solve("solve_b", fold_slab(part_b, owners_b), old_b, inv, mu)
        out_b, _, gram_nb, pack_nb = scale("scale_b", fresh, lax.psum(gram, ALL_AXES), own_b * n_dev, True)
        buf_nb = expand_slab(pack_nb, owners_b)

        plan_c = plan_mode(nblk, nz_vals, at_c, at_a, at_b, rows_c)
        part_c = mttkrp("mttkrp_c", plan_c, buf_a, buf_nb, rows_c)
        inv, mu = invert("invert_c", gram_a, gram_nb)
        fresh, gram = solve("solve_c", fold_slab(part_c, owners_c), old_c, inv, mu)
        out_c, lambdas, _ = scale("scale_c", fresh, lax.psum(gram, ALL_AXES), own_c * n_dev, False)
        return out_a.T, out_b.T, out_c.T, lambdas.reshape(RANK)

    spec_nz = P(("gz", "gy", "gx"))
    spec_a = P(("gx", "gz", "gy"), None)
    spec_b = P(("gy", "gz", "gx"), None)
    spec_c = P(("gz", "gy", "gx"), None)
    return jax.shard_map(
        device_step,
        mesh=mesh,
        in_specs=(spec_nz, spec_nz, spec_nz, spec_nz, spec_a, spec_b, spec_c),
        out_specs=(spec_a, spec_b, spec_c, P()),
        check_vma=False,
    )
```

```python
import functools

import jax
import jax.numpy as jnp
from jax import lax
from jax.experimental import pallas as pl
from jax.experimental.pallas import tpu as pltpu
from jax.sharding import PartitionSpec as P

HIGHEST = lax.Precision.HIGHEST
PROX_WEIGHT = 0.5

LANES = 128
RANK = 64
BLOCK = 1024
UNROLL = 16
STEPS = LANES // UNROLL
CHUNK = 8192
VMEM_MAX = 67_000_000
TAB_STEPS = 8
TAB_SLOTS = 3
OUT_STEPS = 8
WIDEN_ROWS = 32
GATHER_PARTS = 2


def lines_of(own_rows):
    return pl.cdiv(own_rows, 256) * 128


def place_rows(idx, own_rows):
    blk = idx // own_rows
    q = idx - blk * own_rows
    line = blk * lines_of(own_rows) + ((q >> 8) << 7) + (q & 127)
    return line, (q >> 7) & 1


def _bit(n):
    return 1 << n if n < 31 else -(1 << 31)


def mttkrp_body(
    rows_out, rows_one, rows_two, chunk,
    nblk_ref, flag_ref, out_h, one_h, two_h, val_ref, code_ref, line_ref, tab1_h, tab2_h, sum_h,
    acc, acc2, tab1, tab2, stage, raw1a, raw1b, raw2a, raw2b, contrib_a, contrib_b,
    sm_out, sm_one, sm_two, sem_idx, sem_tab, sem_out,
):
    raw1, raw2, contrib = (raw1a, raw1b), (raw2a, raw2b), (contrib_a, contrib_b)
    nblk = nblk_ref[0]
    blk_chunk = chunk // BLOCK
    nchunk = lax.div(nblk + (blk_chunk - 1), blk_chunk)

    def idx_copies(c, slot):
        src = pl.ds(pl.multiple_of(c * chunk, chunk), chunk)
        dst = pl.ds(pl.multiple_of(slot * chunk, chunk), chunk)
        pairs = ((out_h, sm_out), (one_h, sm_one), (two_h, sm_two))
        return [pltpu.make_async_copy(h.at[src], s.at[dst], sem_idx.at[slot, n]) for n, (h, s) in enumerate(pairs)]

    for cp in idx_copies(0, 0):
        cp.start()

    tabs = ((tab1_h, tab1, rows_one // TAB_STEPS), (tab2_h, tab2, rows_two // TAB_STEPS))

    def tab_copy(n):
        tab_h, _, step_rows = tabs[n // TAB_STEPS]
        src = tab_h.at[pl.ds((n % TAB_STEPS) * step_rows, step_rows), :]
        return pltpu.make_async_copy(src, stage.at[n % TAB_SLOTS, pl.ds(0, step_rows), :], sem_tab.at[n % TAB_SLOTS])

    for n in range(TAB_SLOTS):
        tab_copy(n).start()

    def zero(r, _):
        at = pl.ds(pl.multiple_of(r * 128, 128), 128)
        acc[at, :] = jnp.zeros((128, LANES), jnp.float32)
        acc2[at, :] = jnp.zeros((128, LANES), jnp.float32)
        return 0

    lax.fori_loop(0, rows_out // 128, zero, 0)
    acc[pl.ds(rows_out, 16), :] = jnp.zeros((16, LANES), jnp.float32)
    acc2[pl.ds(rows_out, 16), :] = jnp.zeros((16, LANES), jnp.float32)

    for n in range(2 * TAB_STEPS):
        _, tab, step_rows = tabs[n // TAB_STEPS]
        tab_copy(n).wait()

        def widen(r, _, n=n, tab=tab, step_rows=step_rows):
            at = pl.multiple_of(r * WIDEN_ROWS, WIDEN_ROWS)
            dst = pl.ds(pl.multiple_of((n % TAB_STEPS) * step_rows + at, 16), WIDEN_ROWS)
            tab[dst, :] = stage[n % TAB_SLOTS, pl.ds(at, WIDEN_ROWS), :].astype(jnp.float32)
            return 0

        lax.fori_loop(0, step_rows // WIDEN_ROWS, widen, 0)
        if n + TAB_SLOTS < 2 * TAB_STEPS:
            tab_copy(n + TAB_SLOTS).start()

    sub = lax.broadcasted_iota(jnp.int32, (8, LANES), 0)
    lane_id = lax.broadcasted_iota(jnp.int32, (8, LANES), 1)
    right = lane_id >= RANK
    span = 2 * chunk - (7 * 128 + UNROLL - 1)

    def at(sm, s, t):
        return sm.at[pl.ds(128 * s + t, span)]

    def pick(block, lane):
        index = jnp.full((8, LANES), lane, jnp.int32)
        return jnp.take_along_axis(block, index, axis=1, mode="promise_in_bounds")

    def rows8(tab, sm, r, t):
        x = jnp.broadcast_to(tab[pl.ds(at(sm, 0, t)[r], 1), :], (8, LANES))
        for s in range(1, 8):
            row = jnp.broadcast_to(tab[pl.ds(at(sm, s, t)[r], 1), :], (8, LANES))
            x = jnp.where(sub == s, row, x)
        return x

    def gather_group(par, r, t):
        g = slice(8 * t, 8 * t + 8)
        raw1[par][g, :] = rows8(tab1, sm_one, r, t)
        raw2[par][g, :] = rows8(tab2, sm_two, r, t)

    def product_group(par, t, vals, turns, keeps, lane0):
        g = slice(8 * t, 8 * t + 8)
        val = pick(vals, lane0 + t)
        x1, x2 = raw1[par][g, :], raw2[par][g, :]
        x1 = jnp.where((turns & _bit(t)) != 0, pltpu.roll(x1, RANK, axis=1), x1)
        x2 = jnp.where((turns & _bit(16 + t)) != 0, pltpu.roll(x2, RANK, axis=1), x2)
        contrib[par][g, :] = jnp.where((keeps & _bit(t)) != 0, val * (x1 * x2), 0.0)

    def add_group(par, r, t):
        x = contrib[par][8 * t : 8 * t + 8, :]
        row = [at(sm_out, s, t)[r] for s in range(8)]
        dst = acc if t % 2 == 0 else acc2
        sums = [dst[pl.ds(row[s], 8), :] + x for s in range(8)]
        for s in range(8):
            pltpu.store(dst.at[pl.ds(row[s], 8), :], sums[s], mask=(sub == s))

    def merge(par, b, q, flag):
        lines = line_ref[pl.ds(pl.multiple_of(b * 8, 8), 8), :] + sub

        def one(t, _):
            @pl.when((lax.shift_right_logical(flag, t) & 1) == 1)
            def _():
                line = pick(lines, q * UNROLL + t)
                rows = pl.ds(pl.multiple_of(t * 8, 8), 8)
                y = contrib[par][rows, :]
                total = y
                for d in range(1, 8):
                    same = (line == pltpu.roll(line, d, axis=0)) & (sub >= d)
                    total = total + jnp.where(same, pltpu.roll(y, d, axis=0), 0.0)
                contrib[par][rows, :] = total

            return 0

        lax.fori_loop(0, UNROLL, one, 0)

    def chunk_step(c, _):
        slot = lax.rem(c, 2)
        for cp in idx_copies(c, slot):
            cp.wait()

        @pl.when(c + 1 < nchunk)
        def _():
            for cp in idx_copies(c + 1, 1 - slot):
                cp.start()

        n_it = jnp.minimum(blk_chunk, nblk - c * blk_chunk) * STEPS
        last = n_it - 1
        base = slot * chunk

        def place(k):
            bl = k // STEPS
            q = k - bl * STEPS
            return c * blk_chunk + bl, q, base + bl * BLOCK + q * UNROLL

        def block_of(ref, b):
            return ref[pl.ds(pl.multiple_of(b * 8, 8), 8), :]

        def front(k):
            b, q, _ = place(jnp.minimum(k, last))
            codes = block_of(code_ref, b)
            keeps = pick(codes, q + STEPS)
            return block_of(val_ref, b), pick(codes, q), jnp.where(right, keeps, ~keeps), q * UNROLL

        def fetch(par, k):
            _, _, r = place(jnp.minimum(k, last))
            for t in range(UNROLL):
                gather_group(par, r, t)

        fetch(0, 0)
        args0 = front(0)
        for t in range(UNROLL):
            product_group(0, t, *args0)
        fetch(1, 1)

        def step(j, _):
            for par in range(2):
                k = 2 * j + par
                b, q, r = place(k)
                flag = flag_ref[c * (blk_chunk * STEPS) + k]

                @pl.when(flag != 0)
                def _():
                    merge(par, b, q, flag)

                args = front(k + 1)
                _, _, rn = place(jnp.minimum(k + 2, last))
                for t in range(UNROLL):
                    add_group(par, r, t)
                    product_group(1 - par, t, *args)
                    gather_group(par, rn, t)
            return 0

        lax.fori_loop(0, lax.div(n_it, 2), step, 0)
        return 0

    lax.fori_loop(0, nchunk, chunk_step, 0)

    part = rows_out // OUT_STEPS

    def out_copy(n):
        src = acc.at[pl.ds(8 + n * part, part), :]
        return pltpu.make_async_copy(src, sum_h.at[pl.ds(n * part, part), :], sem_out.at[n])

    for n in range(OUT_STEPS):

        def total(r, _, n=n):
            rows = pl.ds(pl.multiple_of(n * part + r * WIDEN_ROWS + 8, 8), WIDEN_ROWS)
            acc[rows, :] = acc[rows, :] + acc2[rows, :]
            return 0

        lax.fori_loop(0, part // WIDEN_ROWS, total, 0)
        out_copy(n).start()
    for n in range(OUT_STEPS):
        out_copy(n).wait()


def mttkrp(name, plan, tab1, tab2, rows_out):
    nblk, flags, line_out, line_one, line_two, vals, code = plan
    nnz = line_out.shape[0]
    rows_one, rows_two = tab1.shape[0], tab2.shape[0]
    chunk = min(CHUNK, nnz)
    stage_rows = max(rows_one, rows_two) // TAB_STEPS
    smem = pl.BlockSpec(memory_space=pltpu.SMEM)
    anym = pl.BlockSpec(memory_space=pl.ANY)
    vmem = pl.BlockSpec(memory_space=pltpu.VMEM)
    tiles = (nnz // LANES, LANES)
    step_buf = pltpu.VMEM((8 * UNROLL, LANES), jnp.float32)
    return pl.pallas_call(
        functools.partial(mttkrp_body, rows_out, rows_one, rows_two, chunk),
        out_shape=jax.ShapeDtypeStruct((rows_out, LANES), jnp.float32),
        in_specs=[smem, smem, anym, anym, anym, vmem, vmem, vmem, anym, anym],
        out_specs=anym,
        scratch_shapes=[
            pltpu.VMEM((rows_out + 16, LANES), jnp.float32),
            pltpu.VMEM((rows_out + 16, LANES), jnp.float32),
            pltpu.VMEM((rows_one, LANES), jnp.float32),
            pltpu.VMEM((rows_two, LANES), jnp.float32),
            pltpu.VMEM((TAB_SLOTS, stage_rows, LANES), jnp.bfloat16),
            *([step_buf] * 6),
            pltpu.SMEM((2 * chunk,), jnp.int32),
            pltpu.SMEM((2 * chunk,), jnp.int32),
            pltpu.SMEM((2 * chunk,), jnp.int32),
            pltpu.SemaphoreType.DMA((2, 3)),
            pltpu.SemaphoreType.DMA((TAB_SLOTS,)),
            pltpu.SemaphoreType.DMA((OUT_STEPS,)),
        ],
        name=name,
        compiler_params=pltpu.CompilerParams(vmem_limit_bytes=VMEM_MAX),
        cost_estimate=pl.CostEstimate(flops=2_000_000_000, bytes_accessed=50_000_000, transcendentals=0),
    )(nblk, flags, line_out, line_one, line_two, vals.reshape(tiles), code, line_out.reshape(tiles), tab1, tab2)


def plan_mode(nblk, nz_vals, out_place, one_place, two_place, rows_out):
    nnz = nz_vals.shape[0]
    shape = (nnz // BLOCK, 8, LANES)
    sub = lax.broadcasted_iota(jnp.int32, shape, 1)
    line = jnp.where(nz_vals != 0, out_place[0], rows_out).reshape(shape)
    repeated = jnp.zeros((shape[0], LANES), jnp.bool_)
    for d in range(1, 8):
        same = (line[:, d:] == line[:, : 8 - d]) & (line[:, d:] != rows_out)
        repeated = repeated | jnp.any(same, axis=1)
    lane = jnp.arange(LANES)
    powers = jnp.where(lane[:, None] // UNROLL == jnp.arange(STEPS)[None, :], 1 << (lane[:, None] % UNROLL), 0)

    def words(bits):
        out = jnp.dot(bits.astype(jnp.bfloat16), powers.astype(jnp.bfloat16), preferred_element_type=jnp.float32)
        return out.astype(jnp.int32)

    rows = (nnz // LANES, LANES)
    half = out_place[1].reshape(rows)
    turn_one = words(one_place[1].reshape(rows) ^ half)
    turn_two = words(two_place[1].reshape(rows) ^ half)
    pad = jnp.zeros((rows[0], LANES - 2 * STEPS), jnp.int32)
    code = jnp.concatenate([turn_one | (turn_two << 16), words(half), pad], axis=1)
    flags = words(repeated).reshape(-1)
    return nblk, flags, (line + 8 - sub).reshape(nnz), one_place[0], two_place[0], nz_vals, code


def dot_t(a, b, dims):
    return lax.dot_general(a, b, (dims, ((), ())), precision=HIGHEST, preferred_element_type=jnp.float32)


def col_tiles(width, body, tail):
    full = width // 256
    if full:
        lax.fori_loop(0, full, lambda t, _: (body(t), 0)[1], 0)
    if width % 256:
        tail(full, width % 256)


def pack_tile(x, out_ref, t):
    w = x.shape[1]
    if w < 256:
        x = jnp.concatenate([x, jnp.zeros((RANK, 256 - w), jnp.float32)], axis=1)
    both = jnp.concatenate([x[:, :128], x[:, 128:]], axis=0)
    at = t * 128 if isinstance(t, int) else pl.multiple_of(t * 128, 128)
    out_ref[pl.ds(at, 128), :] = both.T.astype(jnp.bfloat16)


def cols(ref, t, w):
    at = t * 256 if isinstance(t, int) else pl.multiple_of(t * 256, 256)
    return ref.at[:, pl.ds(at, w)]


def prep_body(b_ref, c_ref, pack_b, pack_c, grams):
    for src, pack, gram in ((b_ref, pack_b, grams.at[:RANK]), (c_ref, pack_c, grams.at[RANK:])):
        gram[...] = jnp.zeros((RANK, RANK), jnp.float32)

        def tile(t, w, src=src, pack=pack, gram=gram):
            x = cols(src, t, w)[...]
            pack_tile(x, pack, t)
            gram[...] += dot_t(x, x, ((1,), (1,)))

        col_tiles(src.shape[1], lambda t: tile(t, 256), tile)


def prep(fac_b_t, fac_c_t):
    packs = [jax.ShapeDtypeStruct((lines_of(f.shape[1]), LANES), jnp.bfloat16) for f in (fac_b_t, fac_c_t)]
    grams = jax.ShapeDtypeStruct((2 * RANK, RANK), jnp.float32)
    return pl.pallas_call(prep_body, out_shape=(*packs, grams), name="prep")(fac_b_t, fac_c_t)


def invert_body(g1_ref, g2_ref, inv_ref, mu_ref, aug):
    order = RANK
    gram = g1_ref[...] * g2_ref[...]
    row_id = lax.broadcasted_iota(jnp.int32, (order, order), 0)
    col_id = lax.broadcasted_iota(jnp.int32, (order, order), 1)
    diag = row_id == col_id
    mu = PROX_WEIGHT * jnp.sum(jnp.where(diag, gram, 0.0), keepdims=True) / order
    mu_ref[...] = jnp.broadcast_to(mu, (8, LANES))
    eye = jnp.where(diag, 1.0, 0.0)
    aug[...] = jnp.concatenate([gram + mu * eye, eye], axis=1)
    rows = lax.broadcasted_iota(jnp.int32, (order, 2 * order), 0)
    lanes = lax.broadcasted_iota(jnp.int32, (order, 2 * order), 1)

    def eliminate(p, _):
        full = aug[...]
        row = aug[pl.ds(p, 1), :]
        col = jnp.sum(jnp.where(lanes == p, full, 0.0), axis=1, keepdims=True)
        pivot = jnp.sum(jnp.where(lanes[:1] == p, row, 0.0), axis=1, keepdims=True)
        row = row / pivot
        aug[...] = jnp.where(rows == p, row, full - col * row)
        return 0

    lax.fori_loop(0, order, eliminate, 0)
    inv_ref[...] = aug[:, order:]


def invert(name, gram_one, gram_two):
    return pl.pallas_call(
        invert_body,
        out_shape=(jax.ShapeDtypeStruct((RANK, RANK), jnp.float32), jax.ShapeDtypeStruct((8, LANES), jnp.float32)),
        scratch_shapes=[pltpu.VMEM((RANK, 2 * RANK), jnp.float32)],
        name=name,
    )(gram_one, gram_two)


def solve_body(m_ref, old_ref, inv_ref, mu_ref, fresh_ref, gram_ref):
    gram_ref[...] = jnp.zeros((RANK, RANK), jnp.float32)
    inv = inv_ref[...]
    mu = mu_ref[:1, :1]

    def tile(t, w):
        at = t * 128 if isinstance(t, int) else pl.multiple_of(t * 128, 128)
        m = m_ref[pl.ds(at, 128), :].T
        m = jnp.concatenate([m[:RANK], m[RANK:]], axis=1)[:, :w]
        y = m + mu * cols(old_ref, t, w)[...]
        x = dot_t(inv, y, ((0,), (0,)))
        cols(fresh_ref, t, w)[...] = x
        gram_ref[...] += dot_t(x, x, ((1,), (1,)))

    col_tiles(old_ref.shape[1], lambda t: tile(t, 256), tile)


def solve(name, m_own, old_t, inv, mu):
    return pl.pallas_call(
        solve_body,
        out_shape=(jax.ShapeDtypeStruct(old_t.shape, jnp.float32), jax.ShapeDtypeStruct((RANK, RANK), jnp.float32)),
        name=name,
    )(m_own, old_t, inv, mu)


def scale_body(total_rows, want_pack, fresh_ref, gram_ref, out_ref, lam_ref, scaled_ref, *pack_ref):
    gram = gram_ref[...]
    row_id = lax.broadcasted_iota(jnp.int32, (RANK, RANK), 0)
    col_id = lax.broadcasted_iota(jnp.int32, (RANK, RANK), 1)
    square = jnp.where(row_id == col_id, gram, 0.0)
    lam_col = jnp.sqrt(jnp.sum(square, axis=1, keepdims=True) / total_rows)
    lam_row = jnp.sqrt(jnp.sum(square, axis=0, keepdims=True) / total_rows)
    lam_ref[...] = lam_row
    scaled_ref[...] = gram / lam_col / lam_row

    def tile(t, w):
        x = cols(fresh_ref, t, w)[...] / lam_col
        cols(out_ref, t, w)[...] = x
        if want_pack:
            pack_tile(x, pack_ref[0], t)

    col_tiles(fresh_ref.shape[1], lambda t: tile(t, 256), tile)


def scale(name, fresh_t, gram_sum, total_rows, want_pack):
    own = fresh_t.shape[1]
    outs = [
        jax.ShapeDtypeStruct(fresh_t.shape, jnp.float32),
        jax.ShapeDtypeStruct((1, RANK), jnp.float32),
        jax.ShapeDtypeStruct((RANK, RANK), jnp.float32),
    ]
    if want_pack:
        outs.append(jax.ShapeDtypeStruct((lines_of(own), LANES), jnp.bfloat16))
    return pl.pallas_call(functools.partial(scale_body, total_rows, want_pack), out_shape=tuple(outs), name=name)(fresh_t, gram_sum)


MESH = pl.DeviceIdType.MESH


def mate_of(minor, width):
    return 1 - minor if width == 2 else lax.rem(minor + 2, 4)


def twin_of(minor):
    return minor + 1 - 2 * lax.rem(minor, 2)


def meet(peers):
    barrier = pltpu.get_barrier_semaphore()
    for peer in peers:
        pl.semaphore_signal(barrier, inc=1, device_id=peer, device_id_type=MESH)
    pl.semaphore_wait(barrier, len(peers))


class Gather:
    def __init__(self, line_axis, n_line, minor_axis, width, own, out, sems):
        self.line_axis, self.n_line, self.minor_axis, self.width = line_axis, n_line, minor_axis, width
        self.own, self.out = own, out
        self.line, self.minor = lax.axis_index(line_axis), lax.axis_index(minor_axis)
        self.local, self.sl, self.rl, self.sp, self.rp, self.sc, self.rc = sems
        self.lines = own.shape[0]
        self.part = self.lines // GATHER_PARTS
        self.cores = width == 4
        self.mate = {minor_axis: mate_of(self.minor, width)}
        self.twin = {minor_axis: twin_of(self.minor)}
        self.others = [lax.rem(self.line + d, n_line) for d in range(1, n_line)]
        self.started = []

    def peers(self):
        return [{self.line_axis: l} for l in self.others] + [self.mate] + ([self.twin] if self.cores else [])

    def rows(self, line, minor, k):
        return self.out.at[pl.ds((line * self.width + minor) * self.lines + k * self.part, self.part), :]

    def send(self, src, dst, send_sem, recv_sem, peer):
        cp = pltpu.make_async_remote_copy(src, dst, send_sem, recv_sem, device_id=peer, device_id_type=MESH)
        cp.start()
        self.started.append(cp)

    def expect(self, dst, recv_sem, send_sem):
        pltpu.make_async_remote_copy(dst, dst, send_sem, recv_sem, device_id=self.mate, device_id_type=MESH).wait_recv()

    def to_mate(self, src, line, k):
        self.send(src, self.rows(line, self.minor, k), self.sp.at[line, k], self.rp.at[line, k], self.mate)

    def to_twin(self, src, line, minor, side, k):
        if self.cores:
            self.send(src, self.rows(line, minor, k), self.sc.at[line, side, k], self.rc.at[line, side, k], self.twin)

    def begin(self):
        for k in range(GATHER_PARTS):
            src = self.own.at[pl.ds(k * self.part, self.part), :]
            self.to_mate(src, self.line, k)
            for l in self.others:
                self.send(src, self.rows(self.line, self.minor, k), self.sl.at[l, k], self.rl.at[self.line, k], {self.line_axis: l})
            self.to_twin(src, self.line, self.minor, 0, k)
        self.keep = pltpu.make_async_copy(self.own, self.out.at[pl.ds((self.line * self.width + self.minor) * self.lines, self.lines), :], self.local)
        self.keep.start()

    def from_line(self, line):
        for k in range(GATHER_PARTS):
            rows = self.rows(line, self.minor, k)
            self.expect(rows, self.rl.at[line, k], self.sl.at[line, k])
            self.to_mate(rows, line, k)
            self.to_twin(rows, line, self.minor, 0, k)

    def from_mate(self, line):
        minor = mate_of(self.minor, self.width)
        for k in range(GATHER_PARTS):
            rows = self.rows(line, minor, k)
            self.expect(rows, self.rp.at[line, k], self.sp.at[line, k])
            self.to_twin(rows, line, minor, 1, k)

    def middle(self):
        order = [lax.rem(self.line + d, self.n_line) for d in range(self.n_line - 1, 0, -1)]
        previous = self.line
        for line in order:
            self.from_line(line)
            self.from_mate(previous)
            previous = line
        self.from_mate(previous)

    def end(self):
        if self.cores:
            twin = twin_of(self.minor)
            for line in [self.line, *self.others]:
                for side, minor in enumerate((twin, mate_of(twin, self.width))):
                    for k in range(GATHER_PARTS):
                        self.expect(self.rows(line, minor, k), self.rc.at[line, side, k], self.sc.at[line, side, k])
        for cp in self.started:
            cp.wait_send()
        self.keep.wait()


def gather_body(specs, *refs):
    n = len(specs)
    owns, outs, sems = refs[:n], refs[n : 2 * n], refs[2 * n :]
    gathers = [Gather(*spec, own, out, sems[7 * i : 7 * i + 7]) for i, (spec, own, out) in enumerate(zip(specs, owns, outs))]
    meet([peer for g in gathers for peer in g.peers()])
    for g in gathers:
        g.begin()
    for g in gathers:
        g.middle()
    for g in gathers:
        g.end()


def expand_slabs(name, collective_id, specs, owns):
    dma = pltpu.SemaphoreType.DMA
    scratch = []
    for _, n_line, _, _ in specs:
        flat, sided = dma((n_line, GATHER_PARTS)), dma((n_line, 2, GATHER_PARTS))
        scratch += [dma, flat, flat, flat, flat, sided, sided]
    outs = [jax.ShapeDtypeStruct((s[1] * s[3] * o.shape[0], LANES), o.dtype) for s, o in zip(specs, owns)]
    return pl.pallas_call(
        functools.partial(gather_body, specs),
        out_shape=tuple(outs),
        in_specs=[pl.BlockSpec(memory_space=pltpu.VMEM)] * len(owns),
        out_specs=tuple([pl.BlockSpec(memory_space=pl.ANY)] * len(owns)),
        scratch_shapes=scratch,
        name=name,
        compiler_params=pltpu.CompilerParams(collective_id=collective_id, has_side_effects=True),
    )(*owns)


def sum_body(sizes, x_ref, out_ref, cur, *rest):
    n = len(sizes)
    slots, sends, recvs = rest[:n], rest[n : 2 * n], rest[2 * n :]
    me = [lax.axis_index(axis) for axis, _ in sizes]
    others = [[lax.rem(m + d, size) for d in range(1, size)] for m, (_, size) in zip(me, sizes)]
    meet([{axis: o} for (axis, _), os in zip(sizes, others) for o in os])
    src = x_ref
    for i, (axis, size) in enumerate(sizes):
        copies = []
        for o in others[i]:
            cp = pltpu.make_async_remote_copy(
                src, slots[i].at[me[i]], sends[i].at[o], recvs[i].at[me[i]], device_id={axis: o}, device_id_type=MESH
            )
            cp.start()
            copies.append(cp)
        slots[i][me[i]] = src[...]
        for o in others[i]:
            pltpu.make_async_remote_copy(
                src, slots[i].at[o], sends[i].at[o], recvs[i].at[o], device_id={axis: o}, device_id_type=MESH
            ).wait_recv()
        total = slots[i][0]
        for k in range(1, size):
            total = total + slots[i][k]
        for cp in copies:
            cp.wait_send()
        dst = out_ref if i == n - 1 else cur.at[i]
        dst[...] = total
        src = dst


def sum_all(name, collective_id, mesh_sizes, x):
    n = len(mesh_sizes)
    dma = pltpu.SemaphoreType.DMA
    scratch = [pltpu.VMEM((n - 1, *x.shape), x.dtype)]
    scratch += [pltpu.VMEM((size, *x.shape), x.dtype) for _, size in mesh_sizes]
    scratch += [dma((size,)) for _, size in mesh_sizes] * 2
    return pl.pallas_call(
        functools.partial(sum_body, mesh_sizes),
        out_shape=jax.ShapeDtypeStruct(x.shape, x.dtype),
        in_specs=[pl.BlockSpec(memory_space=pltpu.VMEM)],
        out_specs=pl.BlockSpec(memory_space=pltpu.VMEM),
        scratch_shapes=scratch,
        name=name,
        compiler_params=pltpu.CompilerParams(collective_id=collective_id, has_side_effects=True),
    )(x)


def fold_slab(part_lines, owner_axes):
    return lax.psum_scatter(part_lines, owner_axes, scatter_dimension=0, tiled=True)


def solution(mesh):
    size_z = mesh.shape["gz"]
    size_y = mesh.shape["gy"]
    size_x = mesh.shape["gx"]
    n_dev = size_z * size_y * size_x
    owners_a = ("gz", "gy")
    owners_b = ("gz", "gx")
    owners_c = ("gy", "gx")

    def device_step(nz_vals, idx_i, idx_j, idx_k, fac_a, fac_b, fac_c):
        own_a, own_b, own_c = fac_a.shape[0], fac_b.shape[0], fac_c.shape[0]
        rows_a = lines_of(own_a) * (n_dev // size_x)
        rows_b = lines_of(own_b) * (n_dev // size_y)
        rows_c = lines_of(own_c) * (n_dev // size_z)
        old_a, old_b, old_c = fac_a.T, fac_b.T, fac_c.T

        sizes = (("gx", size_x), ("gz", size_z), ("gy", size_y))
        spec_a = ("gz", size_z, "gy", size_y)
        spec_b = ("gz", size_z, "gx", size_x)
        spec_c = ("gy", size_y, "gx", size_x)
        pack_b, pack_c, grams = prep(old_b, old_c)
        buf_c, buf_b = expand_slabs("gather_bc", 0, (spec_c, spec_b), (pack_c, pack_b))
        grams = sum_all("sum_bc", 1, sizes, grams)
        gram_b, gram_c = grams[:RANK], grams[RANK:]

        at_a = place_rows(idx_i, own_a)
        at_b = place_rows(idx_j, own_b)
        at_c = place_rows(idx_k, own_c)
        used = jnp.max(jnp.where(nz_vals != 0, jnp.arange(nz_vals.shape[0], dtype=jnp.int32) + 1, 1))
        nblk = ((used + (BLOCK - 1)) // BLOCK).reshape(1)

        plan_a = plan_mode(nblk, nz_vals, at_a, at_b, at_c, rows_a)
        part_a = mttkrp("mttkrp_a", plan_a, buf_b, buf_c, rows_a)
        inv, mu = invert("invert_a", gram_b, gram_c)
        fresh, gram = solve("solve_a", fold_slab(part_a, owners_a), old_a, inv, mu)
        out_a, _, gram_a, pack_a = scale("scale_a", fresh, sum_all("sum_a", 2, sizes, gram), own_a * n_dev, True)
        (buf_a,) = expand_slabs("gather_a", 3, (spec_a,), (pack_a,))

        plan_b = plan_mode(nblk, nz_vals, at_b, at_a, at_c, rows_b)
        part_b = mttkrp("mttkrp_b", plan_b, buf_a, buf_c, rows_b)
        inv, mu = invert("invert_b", gram_a, gram_c)
        fresh, gram = solve("solve_b", fold_slab(part_b, owners_b), old_b, inv, mu)
        out_b, _, gram_nb, pack_nb = scale("scale_b", fresh, sum_all("sum_b", 4, sizes, gram), own_b * n_dev, True)
        (buf_nb,) = expand_slabs("gather_b", 5, (spec_b,), (pack_nb,))

        plan_c = plan_mode(nblk, nz_vals, at_c, at_a, at_b, rows_c)
        part_c = mttkrp("mttkrp_c", plan_c, buf_a, buf_nb, rows_c)
        inv, mu = invert("invert_c", gram_a, gram_nb)
        fresh, gram = solve("solve_c", fold_slab(part_c, owners_c), old_c, inv, mu)
        out_c, lambdas, _ = scale("scale_c", fresh, sum_all("sum_c", 6, sizes, gram), own_c * n_dev, False)
        return out_a.T, out_b.T, out_c.T, lambdas.reshape(RANK)

    part_nz = P(("gz", "gy", "gx"))
    part_a = P(("gx", "gz", "gy"), None)
    part_b = P(("gy", "gz", "gx"), None)
    part_c = P(("gz", "gy", "gx"), None)
    return jax.shard_map(
        device_step,
        mesh=mesh,
        in_specs=(part_nz, part_nz, part_nz, part_nz, part_a, part_b, part_c),
        out_specs=(part_a, part_b, part_c, P()),
        check_vma=False,
    )
```

```python
import functools
import itertools
import math

import jax
import jax.numpy as jnp
from jax import lax
from jax.experimental import pallas as pl
from jax.experimental.pallas import tpu as pltpu
from jax.sharding import PartitionSpec as P

HIGHEST = lax.Precision.HIGHEST
PROX_WEIGHT = 0.5

LANES = 128
RANK = 64
BLOCK = 1024
UNROLL = 16
STEPS = LANES // UNROLL
CHUNK = 8192
VMEM_MAX = 67_000_000
TAB_STEPS = 8
TAB_SLOTS = 3
OUT_STEPS = 8
WIDEN_ROWS = 32
GATHER_PARTS = 4
FOLD_LAG = 2


def lines_of(own_rows):
    return pl.cdiv(own_rows, 256) * 128


def place_rows(idx, own_rows):
    blk = idx // own_rows
    q = idx - blk * own_rows
    line = blk * lines_of(own_rows) + ((q >> 8) << 7) + (q & 127)
    return line, (q >> 7) & 1


def _bit(n):
    return 1 << n if n < 31 else -(1 << 31)


def mttkrp_body(
    rows_out, rows_one, rows_two, chunk,
    nblk_ref, flag_ref, out_h, one_h, two_h, val_ref, code_ref, line_ref, tab1_h, tab2_h, sum_h,
    acc, acc2, tab1, tab2, stage, raw1a, raw1b, raw2a, raw2b, contrib_a, contrib_b,
    sm_out, sm_one, sm_two, sem_idx, sem_tab, sem_out,
):
    raw1, raw2, contrib = (raw1a, raw1b), (raw2a, raw2b), (contrib_a, contrib_b)
    nblk = nblk_ref[0]
    blk_chunk = chunk // BLOCK
    nchunk = lax.div(nblk + (blk_chunk - 1), blk_chunk)

    def idx_copies(c, slot):
        src = pl.ds(pl.multiple_of(c * chunk, chunk), chunk)
        dst = pl.ds(pl.multiple_of(slot * chunk, chunk), chunk)
        pairs = ((out_h, sm_out), (one_h, sm_one), (two_h, sm_two))
        return [pltpu.make_async_copy(h.at[src], s.at[dst], sem_idx.at[slot, n]) for n, (h, s) in enumerate(pairs)]

    for cp in idx_copies(0, 0):
        cp.start()

    tabs = ((tab1_h, tab1, rows_one // TAB_STEPS), (tab2_h, tab2, rows_two // TAB_STEPS))

    def tab_copy(n):
        tab_h, _, step_rows = tabs[n // TAB_STEPS]
        src = tab_h.at[pl.ds((n % TAB_STEPS) * step_rows, step_rows), :]
        return pltpu.make_async_copy(src, stage.at[n % TAB_SLOTS, pl.ds(0, step_rows), :], sem_tab.at[n % TAB_SLOTS])

    for n in range(TAB_SLOTS):
        tab_copy(n).start()

    def zero(r, _):
        at = pl.ds(pl.multiple_of(r * 128, 128), 128)
        acc[at, :] = jnp.zeros((128, LANES), jnp.float32)
        acc2[at, :] = jnp.zeros((128, LANES), jnp.float32)
        return 0

    lax.fori_loop(0, rows_out // 128, zero, 0)
    acc[pl.ds(rows_out, 16), :] = jnp.zeros((16, LANES), jnp.float32)
    acc2[pl.ds(rows_out, 16), :] = jnp.zeros((16, LANES), jnp.float32)

    for n in range(2 * TAB_STEPS):
        _, tab, step_rows = tabs[n // TAB_STEPS]
        tab_copy(n).wait()

        def widen(r, _, n=n, tab=tab, step_rows=step_rows):
            at = pl.multiple_of(r * WIDEN_ROWS, WIDEN_ROWS)
            dst = pl.ds(pl.multiple_of((n % TAB_STEPS) * step_rows + at, 16), WIDEN_ROWS)
            tab[dst, :] = stage[n % TAB_SLOTS, pl.ds(at, WIDEN_ROWS), :].astype(jnp.float32)
            return 0

        lax.fori_loop(0, step_rows // WIDEN_ROWS, widen, 0)
        if n + TAB_SLOTS < 2 * TAB_STEPS:
            tab_copy(n + TAB_SLOTS).start()

    sub = lax.broadcasted_iota(jnp.int32, (8, LANES), 0)
    lane_id = lax.broadcasted_iota(jnp.int32, (8, LANES), 1)
    right = lane_id >= RANK
    span = 2 * chunk - (7 * 128 + UNROLL - 1)

    def at(sm, s, t):
        return sm.at[pl.ds(128 * s + t, span)]

    def pick(block, lane):
        index = jnp.full((8, LANES), lane, jnp.int32)
        return jnp.take_along_axis(block, index, axis=1, mode="promise_in_bounds")

    def rows8(tab, sm, r, t):
        x = jnp.broadcast_to(tab[pl.ds(at(sm, 0, t)[r], 1), :], (8, LANES))
        for s in range(1, 8):
            row = jnp.broadcast_to(tab[pl.ds(at(sm, s, t)[r], 1), :], (8, LANES))
            x = jnp.where(sub == s, row, x)
        return x

    def gather_group(par, r, t):
        g = slice(8 * t, 8 * t + 8)
        raw1[par][g, :] = rows8(tab1, sm_one, r, t)
        raw2[par][g, :] = rows8(tab2, sm_two, r, t)

    def product_group(par, t, vals, turns, keeps, lane0):
        g = slice(8 * t, 8 * t + 8)
        val = pick(vals, lane0 + t)
        x1, x2 = raw1[par][g, :], raw2[par][g, :]
        x1 = jnp.where((turns & _bit(t)) != 0, pltpu.roll(x1, RANK, axis=1), x1)
        x2 = jnp.where((turns & _bit(16 + t)) != 0, pltpu.roll(x2, RANK, axis=1), x2)
        contrib[par][g, :] = jnp.where((keeps & _bit(t)) != 0, val * (x1 * x2), 0.0)

    def add_group(par, r, t):
        x = contrib[par][8 * t : 8 * t + 8, :]
        row = [at(sm_out, s, t)[r] for s in range(8)]
        dst = acc if t % 2 == 0 else acc2
        sums = [dst[pl.ds(row[s], 8), :] + x for s in range(8)]
        for s in range(8):
            pltpu.store(dst.at[pl.ds(row[s], 8), :], sums[s], mask=(sub == s))

    def merge(par, b, q, flag):
        lines = line_ref[pl.ds(pl.multiple_of(b * 8, 8), 8), :] + sub

        def one(t, _):
            @pl.when((lax.shift_right_logical(flag, t) & 1) == 1)
            def _():
                line = pick(lines, q * UNROLL + t)
                rows = pl.ds(pl.multiple_of(t * 8, 8), 8)
                y = contrib[par][rows, :]
                total = y
                for d in range(1, 8):
                    same = (line == pltpu.roll(line, d, axis=0)) & (sub >= d)
                    total = total + jnp.where(same, pltpu.roll(y, d, axis=0), 0.0)
                contrib[par][rows, :] = total

            return 0

        lax.fori_loop(0, UNROLL, one, 0)

    def chunk_step(c, _):
        slot = lax.rem(c, 2)
        for cp in idx_copies(c, slot):
            cp.wait()

        @pl.when(c + 1 < nchunk)
        def _():
            for cp in idx_copies(c + 1, 1 - slot):
                cp.start()

        n_it = jnp.minimum(blk_chunk, nblk - c * blk_chunk) * STEPS
        last = n_it - 1
        base = slot * chunk

        def place(k):
            bl = k // STEPS
            q = k - bl * STEPS
            return c * blk_chunk + bl, q, base + bl * BLOCK + q * UNROLL

        def block_of(ref, b):
            return ref[pl.ds(pl.multiple_of(b * 8, 8), 8), :]

        def front(k):
            b, q, _ = place(jnp.minimum(k, last))
            codes = block_of(code_ref, b)
            keeps = pick(codes, q + STEPS)
            return block_of(val_ref, b), pick(codes, q), jnp.where(right, keeps, ~keeps), q * UNROLL

        def fetch(par, k):
            _, _, r = place(jnp.minimum(k, last))
            for t in range(UNROLL):
                gather_group(par, r, t)

        fetch(0, 0)
        args0 = front(0)
        for t in range(UNROLL):
            product_group(0, t, *args0)
        fetch(1, 1)

        def step(j, _):
            for par in range(2):
                k = 2 * j + par
                b, q, r = place(k)
                flag = flag_ref[c * (blk_chunk * STEPS) + k]

                @pl.when(flag != 0)
                def _():
                    merge(par, b, q, flag)

                args = front(k + 1)
                _, _, rn = place(jnp.minimum(k + 2, last))
                for t in range(UNROLL):
                    add_group(par, r, t)
                    product_group(1 - par, t, *args)
                    gather_group(par, rn, t)
            return 0

        lax.fori_loop(0, lax.div(n_it, 2), step, 0)
        return 0

    lax.fori_loop(0, nchunk, chunk_step, 0)

    part = rows_out // OUT_STEPS

    def out_copy(n):
        src = acc.at[pl.ds(8 + n * part, part), :]
        return pltpu.make_async_copy(src, sum_h.at[pl.ds(n * part, part), :], sem_out.at[n])

    for n in range(OUT_STEPS):

        def total(r, _, n=n):
            rows = pl.ds(pl.multiple_of(n * part + r * WIDEN_ROWS + 8, 8), WIDEN_ROWS)
            acc[rows, :] = acc[rows, :] + acc2[rows, :]
            return 0

        lax.fori_loop(0, part // WIDEN_ROWS, total, 0)
        out_copy(n).start()
    for n in range(OUT_STEPS):
        out_copy(n).wait()


def mttkrp(name, plan, tab1, tab2, rows_out):
    nblk, flags, line_out, line_one, line_two, vals, code = plan
    nnz = line_out.shape[0]
    rows_one, rows_two = tab1.shape[0], tab2.shape[0]
    chunk = min(CHUNK, nnz)
    stage_rows = max(rows_one, rows_two) // TAB_STEPS
    smem = pl.BlockSpec(memory_space=pltpu.SMEM)
    anym = pl.BlockSpec(memory_space=pl.ANY)
    vmem = pl.BlockSpec(memory_space=pltpu.VMEM)
    tiles = (nnz // LANES, LANES)
    step_buf = pltpu.VMEM((8 * UNROLL, LANES), jnp.float32)
    return pl.pallas_call(
        functools.partial(mttkrp_body, rows_out, rows_one, rows_two, chunk),
        out_shape=jax.ShapeDtypeStruct((rows_out, LANES), jnp.float32),
        in_specs=[smem, smem, anym, anym, anym, vmem, vmem, vmem, anym, anym],
        out_specs=anym,
        scratch_shapes=[
            pltpu.VMEM((rows_out + 16, LANES), jnp.float32),
            pltpu.VMEM((rows_out + 16, LANES), jnp.float32),
            pltpu.VMEM((rows_one, LANES), jnp.float32),
            pltpu.VMEM((rows_two, LANES), jnp.float32),
            pltpu.VMEM((TAB_SLOTS, stage_rows, LANES), jnp.bfloat16),
            *([step_buf] * 6),
            pltpu.SMEM((2 * chunk,), jnp.int32),
            pltpu.SMEM((2 * chunk,), jnp.int32),
            pltpu.SMEM((2 * chunk,), jnp.int32),
            pltpu.SemaphoreType.DMA((2, 3)),
            pltpu.SemaphoreType.DMA((TAB_SLOTS,)),
            pltpu.SemaphoreType.DMA((OUT_STEPS,)),
        ],
        name=name,
        compiler_params=pltpu.CompilerParams(vmem_limit_bytes=VMEM_MAX),
        cost_estimate=pl.CostEstimate(flops=2_000_000_000, bytes_accessed=50_000_000, transcendentals=0),
    )(nblk, flags, line_out, line_one, line_two, vals.reshape(tiles), code, line_out.reshape(tiles), tab1, tab2)


def plan_mode(nblk, nz_vals, out_place, one_place, two_place, rows_out):
    nnz = nz_vals.shape[0]
    shape = (nnz // BLOCK, 8, LANES)
    sub = lax.broadcasted_iota(jnp.int32, shape, 1)
    line = jnp.where(nz_vals != 0, out_place[0], rows_out).reshape(shape)
    repeated = jnp.zeros((shape[0], LANES), jnp.bool_)
    for d in range(1, 8):
        same = (line[:, d:] == line[:, : 8 - d]) & (line[:, d:] != rows_out)
        repeated = repeated | jnp.any(same, axis=1)
    lane = jnp.arange(LANES)
    powers = jnp.where(lane[:, None] // UNROLL == jnp.arange(STEPS)[None, :], 1 << (lane[:, None] % UNROLL), 0)

    def words(bits):
        out = jnp.dot(bits.astype(jnp.bfloat16), powers.astype(jnp.bfloat16), preferred_element_type=jnp.float32)
        return out.astype(jnp.int32)

    rows = (nnz // LANES, LANES)
    half = out_place[1].reshape(rows)
    turn_one = words(one_place[1].reshape(rows) ^ half)
    turn_two = words(two_place[1].reshape(rows) ^ half)
    pad = jnp.zeros((rows[0], LANES - 2 * STEPS), jnp.int32)
    code = jnp.concatenate([turn_one | (turn_two << 16), words(half), pad], axis=1)
    flags = words(repeated).reshape(-1)
    return nblk, flags, (line + 8 - sub).reshape(nnz), one_place[0], two_place[0], nz_vals, code


def dot_t(a, b, dims):
    return lax.dot_general(a, b, (dims, ((), ())), precision=HIGHEST, preferred_element_type=jnp.float32)


def col_tiles(width, body, tail):
    full = width // 256
    if full:
        lax.fori_loop(0, full, lambda t, _: (body(t), 0)[1], 0)
    if width % 256:
        tail(full, width % 256)


def pack_tile(x, out_ref, t):
    w = x.shape[1]
    if w < 256:
        x = jnp.concatenate([x, jnp.zeros((RANK, 256 - w), jnp.float32)], axis=1)
    both = jnp.concatenate([x[:, :128], x[:, 128:]], axis=0)
    at = t * 128 if isinstance(t, int) else pl.multiple_of(t * 128, 128)
    out_ref[pl.ds(at, 128), :] = both.T.astype(jnp.bfloat16)


def cols(ref, t, w):
    at = t * 256 if isinstance(t, int) else pl.multiple_of(t * 256, 256)
    return ref.at[:, pl.ds(at, w)]


def prep_body(b_ref, c_ref, pack_b, pack_c, grams):
    for src, pack, gram in ((b_ref, pack_b, grams.at[:RANK]), (c_ref, pack_c, grams.at[RANK:])):
        gram[...] = jnp.zeros((RANK, RANK), jnp.float32)

        def tile(t, w, src=src, pack=pack, gram=gram):
            x = cols(src, t, w)[...]
            pack_tile(x, pack, t)
            gram[...] += dot_t(x, x, ((1,), (1,)))

        col_tiles(src.shape[1], lambda t: tile(t, 256), tile)


def prep(fac_b_t, fac_c_t):
    packs = [jax.ShapeDtypeStruct((lines_of(f.shape[1]), LANES), jnp.bfloat16) for f in (fac_b_t, fac_c_t)]
    grams = jax.ShapeDtypeStruct((2 * RANK, RANK), jnp.float32)
    return pl.pallas_call(prep_body, out_shape=(*packs, grams), name="prep")(fac_b_t, fac_c_t)


def invert_body(g1_ref, g2_ref, inv_ref, mu_ref, aug):
    order = RANK
    gram = g1_ref[...] * g2_ref[...]
    row_id = lax.broadcasted_iota(jnp.int32, (order, order), 0)
    col_id = lax.broadcasted_iota(jnp.int32, (order, order), 1)
    diag = row_id == col_id
    mu = PROX_WEIGHT * jnp.sum(jnp.where(diag, gram, 0.0), keepdims=True) / order
    mu_ref[...] = jnp.broadcast_to(mu, (8, LANES))
    eye = jnp.where(diag, 1.0, 0.0)
    aug[...] = jnp.concatenate([gram + mu * eye, eye], axis=1)
    rows = lax.broadcasted_iota(jnp.int32, (order, 2 * order), 0)
    lanes = lax.broadcasted_iota(jnp.int32, (order, 2 * order), 1)

    def eliminate(p, _):
        full = aug[...]
        row = aug[pl.ds(p, 1), :]
        col = jnp.sum(jnp.where(lanes == p, full, 0.0), axis=1, keepdims=True)
        pivot = jnp.sum(jnp.where(lanes[:1] == p, row, 0.0), axis=1, keepdims=True)
        row = row / pivot
        aug[...] = jnp.where(rows == p, row, full - col * row)
        return 0

    lax.fori_loop(0, order, eliminate, 0)
    inv_ref[...] = aug[:, order:]


def invert(name, gram_one, gram_two):
    return pl.pallas_call(
        invert_body,
        out_shape=(jax.ShapeDtypeStruct((RANK, RANK), jnp.float32), jax.ShapeDtypeStruct((8, LANES), jnp.float32)),
        scratch_shapes=[pltpu.VMEM((RANK, 2 * RANK), jnp.float32)],
        name=name,
    )(gram_one, gram_two)


def solve_body(m_ref, old_ref, inv_ref, mu_ref, fresh_ref, gram_ref):
    gram_ref[...] = jnp.zeros((RANK, RANK), jnp.float32)
    inv = inv_ref[...]
    mu = mu_ref[:1, :1]

    def tile(t, w):
        at = t * 128 if isinstance(t, int) else pl.multiple_of(t * 128, 128)
        m = m_ref[pl.ds(at, 128), :].T
        m = jnp.concatenate([m[:RANK], m[RANK:]], axis=1)[:, :w]
        y = m + mu * cols(old_ref, t, w)[...]
        x = dot_t(inv, y, ((0,), (0,)))
        cols(fresh_ref, t, w)[...] = x
        gram_ref[...] += dot_t(x, x, ((1,), (1,)))

    col_tiles(old_ref.shape[1], lambda t: tile(t, 256), tile)


def solve(name, m_own, old_t, inv, mu):
    return pl.pallas_call(
        solve_body,
        out_shape=(jax.ShapeDtypeStruct(old_t.shape, jnp.float32), jax.ShapeDtypeStruct((RANK, RANK), jnp.float32)),
        name=name,
    )(m_own, old_t, inv, mu)


def scale_body(total_rows, want_pack, fresh_ref, gram_ref, out_ref, lam_ref, scaled_ref, *pack_ref):
    gram = gram_ref[...]
    row_id = lax.broadcasted_iota(jnp.int32, (RANK, RANK), 0)
    col_id = lax.broadcasted_iota(jnp.int32, (RANK, RANK), 1)
    square = jnp.where(row_id == col_id, gram, 0.0)
    lam_col = jnp.sqrt(jnp.sum(square, axis=1, keepdims=True) / total_rows)
    lam_row = jnp.sqrt(jnp.sum(square, axis=0, keepdims=True) / total_rows)
    lam_ref[...] = lam_row
    scaled_ref[...] = gram / lam_col / lam_row

    def tile(t, w):
        x = cols(fresh_ref, t, w)[...] / lam_col
        cols(out_ref, t, w)[...] = x
        if want_pack:
            pack_tile(x, pack_ref[0], t)

    col_tiles(fresh_ref.shape[1], lambda t: tile(t, 256), tile)


def scale(name, fresh_t, gram_sum, total_rows, want_pack):
    own = fresh_t.shape[1]
    outs = [
        jax.ShapeDtypeStruct(fresh_t.shape, jnp.float32),
        jax.ShapeDtypeStruct((1, RANK), jnp.float32),
        jax.ShapeDtypeStruct((RANK, RANK), jnp.float32),
    ]
    if want_pack:
        outs.append(jax.ShapeDtypeStruct((lines_of(own), LANES), jnp.bfloat16))
    return pl.pallas_call(functools.partial(scale_body, total_rows, want_pack), out_shape=tuple(outs), name=name)(fresh_t, gram_sum)


MESH = pl.DeviceIdType.MESH


def mate_of(minor, width):
    return 1 - minor if width == 2 else lax.rem(minor + 2, 4)


def twin_of(minor):
    return minor + 1 - 2 * lax.rem(minor, 2)


def meet(peers):
    barrier = pltpu.get_barrier_semaphore()
    for peer in peers:
        pl.semaphore_signal(barrier, inc=1, device_id=peer, device_id_type=MESH)
    pl.semaphore_wait(barrier, len(peers))


class Gather:
    def __init__(self, line_axis, n_line, minor_axis, width, own, out, sems):
        self.line_axis, self.n_line, self.minor_axis, self.width = line_axis, n_line, minor_axis, width
        self.own, self.out = own, out
        self.line, self.minor = lax.axis_index(line_axis), lax.axis_index(minor_axis)
        self.local, self.sl, self.rl, self.sp, self.rp, self.sc, self.rc = sems
        self.lines = own.shape[0]
        self.part = self.lines // GATHER_PARTS
        self.cores = width == 4
        self.mate = {minor_axis: mate_of(self.minor, width)}
        self.twin = {minor_axis: twin_of(self.minor)}
        self.others = [lax.rem(self.line + d, n_line) for d in range(1, n_line)]
        self.started = []

    def peers(self):
        return [{self.line_axis: l} for l in self.others] + [self.mate] + ([self.twin] if self.cores else [])

    def rows(self, line, minor, k):
        return self.out.at[pl.ds((line * self.width + minor) * self.lines + k * self.part, self.part), :]

    def send(self, src, dst, send_sem, recv_sem, peer):
        cp = pltpu.make_async_remote_copy(src, dst, send_sem, recv_sem, device_id=peer, device_id_type=MESH)
        cp.start()
        self.started.append(cp)

    def expect(self, dst, recv_sem, send_sem):
        pltpu.make_async_remote_copy(dst, dst, send_sem, recv_sem, device_id=self.mate, device_id_type=MESH).wait_recv()

    def to_mate(self, src, line, k):
        self.send(src, self.rows(line, self.minor, k), self.sp.at[line, k], self.rp.at[line, k], self.mate)

    def to_twin(self, src, line, minor, side, k):
        if self.cores:
            self.send(src, self.rows(line, minor, k), self.sc.at[line, side, k], self.rc.at[line, side, k], self.twin)

    def begin(self):
        for k in range(GATHER_PARTS):
            src = self.own.at[pl.ds(k * self.part, self.part), :]
            self.to_mate(src, self.line, k)
            for l in self.others:
                self.send(src, self.rows(self.line, self.minor, k), self.sl.at[l, k], self.rl.at[self.line, k], {self.line_axis: l})
            self.to_twin(src, self.line, self.minor, 0, k)
        self.keep = pltpu.make_async_copy(self.own, self.out.at[pl.ds((self.line * self.width + self.minor) * self.lines, self.lines), :], self.local)
        self.keep.start()

    def from_line(self, line):
        for k in range(GATHER_PARTS):
            rows = self.rows(line, self.minor, k)
            self.expect(rows, self.rl.at[line, k], self.sl.at[line, k])
            self.to_mate(rows, line, k)
            self.to_twin(rows, line, self.minor, 0, k)

    def from_mate(self, line):
        minor = mate_of(self.minor, self.width)
        for k in range(GATHER_PARTS):
            rows = self.rows(line, minor, k)
            self.expect(rows, self.rp.at[line, k], self.sp.at[line, k])
            self.to_twin(rows, line, minor, 1, k)

    def middle(self):
        order = [lax.rem(self.line + d, self.n_line) for d in range(self.n_line - 1, 0, -1)]
        previous = self.line
        for line in order:
            self.from_line(line)
            self.from_mate(previous)
            previous = line
        self.from_mate(previous)

    def end(self):
        if self.cores:
            twin = twin_of(self.minor)
            for line in [self.line, *self.others]:
                for side, minor in enumerate((twin, mate_of(twin, self.width))):
                    for k in range(GATHER_PARTS):
                        self.expect(self.rows(line, minor, k), self.rc.at[line, side, k], self.sc.at[line, side, k])
        for cp in self.started:
            cp.wait_send()
        self.keep.wait()


def gather_body(specs, *refs):
    n = len(specs)
    owns, outs, sems = refs[:n], refs[n : 2 * n], refs[2 * n :]
    gathers = [Gather(*spec, own, out, sems[7 * i : 7 * i + 7]) for i, (spec, own, out) in enumerate(zip(specs, owns, outs))]
    meet([peer for g in gathers for peer in g.peers()])
    for g in gathers:
        g.begin()
    for g in gathers:
        g.middle()
    for g in gathers:
        g.end()


def expand_slabs(name, collective_id, specs, owns):
    dma = pltpu.SemaphoreType.DMA
    scratch = []
    for _, n_line, _, _ in specs:
        flat, sided = dma((n_line, GATHER_PARTS)), dma((n_line, 2, GATHER_PARTS))
        scratch += [dma, flat, flat, flat, flat, sided, sided]
    outs = [jax.ShapeDtypeStruct((s[1] * s[3] * o.shape[0], LANES), o.dtype) for s, o in zip(specs, owns)]
    return pl.pallas_call(
        functools.partial(gather_body, specs),
        out_shape=tuple(outs),
        in_specs=[pl.BlockSpec(memory_space=pltpu.VMEM)] * len(owns),
        out_specs=tuple([pl.BlockSpec(memory_space=pl.ANY)] * len(owns)),
        scratch_shapes=scratch,
        name=name,
        compiler_params=pltpu.CompilerParams(collective_id=collective_id, has_side_effects=True),
    )(*owns)


def sum_body(sizes, x_ref, out_ref, cur, *rest):
    n = len(sizes)
    slots, sends, recvs = rest[:n], rest[n : 2 * n], rest[2 * n :]
    me = [lax.axis_index(axis) for axis, _ in sizes]
    others = [[lax.rem(m + d, size) for d in range(1, size)] for m, (_, size) in zip(me, sizes)]
    meet([{axis: o} for (axis, _), os in zip(sizes, others) for o in os])
    src = x_ref
    for i, (axis, size) in enumerate(sizes):
        copies = []
        for o in others[i]:
            cp = pltpu.make_async_remote_copy(
                src, slots[i].at[me[i]], sends[i].at[o], recvs[i].at[me[i]], device_id={axis: o}, device_id_type=MESH
            )
            cp.start()
            copies.append(cp)
        slots[i][me[i]] = src[...]
        for o in others[i]:
            pltpu.make_async_remote_copy(
                src, slots[i].at[o], sends[i].at[o], recvs[i].at[o], device_id={axis: o}, device_id_type=MESH
            ).wait_recv()
        total = slots[i][0]
        for k in range(1, size):
            total = total + slots[i][k]
        for cp in copies:
            cp.wait_send()
        dst = out_ref if i == n - 1 else cur.at[i]
        dst[...] = total
        src = dst


def sum_all(name, collective_id, mesh_sizes, x):
    n = len(mesh_sizes)
    dma = pltpu.SemaphoreType.DMA
    scratch = [pltpu.VMEM((n - 1, *x.shape), x.dtype)]
    scratch += [pltpu.VMEM((size, *x.shape), x.dtype) for _, size in mesh_sizes]
    scratch += [dma((size,)) for _, size in mesh_sizes] * 2
    return pl.pallas_call(
        functools.partial(sum_body, mesh_sizes),
        out_shape=jax.ShapeDtypeStruct(x.shape, x.dtype),
        in_specs=[pl.BlockSpec(memory_space=pltpu.VMEM)],
        out_specs=pl.BlockSpec(memory_space=pltpu.VMEM),
        scratch_shapes=scratch,
        name=name,
        compiler_params=pltpu.CompilerParams(collective_id=collective_id, has_side_effects=True),
    )(x)


class Fold:
    def __init__(self, dims, colors, pieces, x, own, out, bufs, sends, recvs, local):
        self.dims, self.colors, self.pieces = dims, colors, pieces
        self.names = [name for name, _ in dims]
        self.size = dict(dims)
        self.x, self.own, self.out, self.local = x, own, out, local
        gx = lax.axis_index("gx")
        self.at = {"z": lax.axis_index("gz"), "y": lax.axis_index("gy"), "x": lax.div(gx, 2), "c": lax.rem(gx, 2)}
        self.flows = []
        first_line, n = 0, 0
        for order, lines in colors:
            off = 0
            for j, name in enumerate(order):
                lag = 1 if name == "c" else FOLD_LAG
                for way in (1, -1):
                    self.flows.append((order, j, lines, first_line, off, lag, way, bufs[n], sends.at[n], recvs.at[n]))
                    n += 1
                off += lag * (self.size[name] - 1)
            first_line += lines * pieces
            self.last = off

    def peer(self, name, pos):
        if name == "z":
            return {"gz": pos}
        if name == "y":
            return {"gy": pos}
        return {"gx": pos * 2 + self.at["c"] if name == "x" else self.at["x"] * 2 + pos}

    def peers(self):
        found = []
        for name, size in self.dims:
            found += [self.peer(name, lax.rem(self.at[name] + d, size)) for d in range(1, size)]
        return found

    def view(self, ref, order, j, current, lines):
        index = [self.at[d] if d in order[:j] else current if d == order[j] else slice(None) for d in self.names]
        return ref.at[(*index, lines, slice(None))]

    def slot(self, buf, order, j, current, lines):
        left = [d for d in self.names if d not in order[:j]]
        return buf.at[(*[current if d == order[j] else slice(None) for d in left], lines, slice(None))]

    def rows(self, flow, c):
        _, _, lines, first, *_ = flow
        return pl.ds(pl.multiple_of(first + c * lines, 8), lines), pl.ds(pl.multiple_of(c * lines, 8), lines)

    def copy(self, flow, p, c):
        order, j, _, _, _, _, way, buf, send, recv = flow
        n = self.size[order[j]]
        count = n - 1 - p if way > 0 else p
        mine, theirs = self.rows(flow, c)
        blocks = slice(p + 1, n) if way > 0 else slice(0, p)
        src = self.view(self.x if j == 0 and count == n - 1 else self.own, order, j, blocks, mine)
        dst = self.slot(buf, order, j, slice(0, count), theirs)
        return pltpu.make_async_remote_copy(
            src, dst, send.at[c], recv.at[c], device_id=self.peer(order[j], p + way), device_id_type=MESH
        )

    def take(self, flow, p, c):
        order, j, _, _, _, _, way, buf, send, recv = flow
        n = self.size[order[j]]
        count = n - p if way > 0 else p + 1
        first = p if way > 0 else 0
        mine, theirs = self.rows(flow, c)
        dst = self.slot(buf, order, j, slice(0, count), theirs)
        pltpu.make_async_remote_copy(
            dst, dst, send.at[c], recv.at[c], device_id=self.peer(order[j], p - way), device_id_type=MESH
        ).wait_recv()
        left = [d for d in self.names if d not in order[:j]]
        for place in itertools.product(*[range(count if d == order[j] else self.size[d]) for d in left]):
            spot = dict(zip(left, place))
            at = [self.at[d] if d in order[:j] else spot[d] + (first if d == order[j] else 0) for d in self.names]
            at = (*at, mine, slice(None))
            self.own[at] = self.own[at] + buf[(*place, theirs, slice(None))]

    def each(self, s, act, wants):
        for flow in self.flows:
            order, j, _, _, off, lag, way = flow[:7]
            n = self.size[order[j]]
            for p in range(n):
                hop = p if way > 0 else n - 1 - p
                if not wants(hop, n):
                    continue
                c = s - off - lag * hop

                @pl.when((self.at[order[j]] == p) & (c >= 0) & (c < self.pieces))
                def _(flow=flow, p=p, c=c):
                    act(flow, p, c)

    def run(self):
        load = pltpu.make_async_copy(self.x, self.own, self.local)
        load.start()
        steps = self.pieces + self.last
        sends = lambda hop, n: hop < n - 1
        takes = lambda hop, n: hop > 0

        def step(s, _):
            @pl.when(s == 1)
            def _():
                load.wait()

            self.each(s, self.take, takes)
            self.each(s, lambda f, p, c: self.copy(f, p, c).start(), sends)
            return 0

        lax.fori_loop(0, steps, step, 0)
        index = tuple(self.at[d] for d in self.names)
        keep = pltpu.make_async_copy(self.own.at[index], self.out, self.local)
        keep.start()

        def drain(s, _):
            self.each(s, lambda f, p, c: self.copy(f, p, c).wait_send(), sends)
            return 0

        lax.fori_loop(0, steps, drain, 0)
        keep.wait()


def fold_body(dims, colors, pieces, n_flows, x, out, own, *rest):
    bufs, (sends, recvs, local) = rest[:n_flows], rest[n_flows:]
    fold = Fold(dims, colors, pieces, x, own, out, bufs, sends, recvs, local)
    meet(fold.peers())
    fold.run()


def fold_plan(kind, lines):
    if kind == "a":
        dims, orders, share = (("z", 4), ("y", 2)), (("y", "z"), ("z", "y")), (56, 8)
    elif kind == "b":
        dims, orders, share = (("z", 4), ("x", 2), ("c", 2)), (("c", "x", "z"), ("c", "z", "x")), (24, 8)
    else:
        dims, orders, share = (("y", 2), ("x", 2), ("c", 2)), (("c", "x", "y"), ("c", "y", "x")), (32, 32)
    return dims, tuple(zip(orders, share)), lines // sum(share)


def fold_slab(name, collective_id, kind, part_lines):
    dims, _, _ = fold_plan(kind, 0)
    grid = tuple(size for _, size in dims)
    lines = part_lines.shape[0] // math.prod(grid)
    dims, colors, pieces = fold_plan(kind, lines)
    size = dict(dims)
    bufs = []
    for order, share in colors:
        for j, axis in enumerate(order):
            left = [size[d] - (d == axis) for d, _ in dims if d not in order[:j]]
            bufs += [pltpu.VMEM((*left, share * pieces, LANES), jnp.float32)] * 2
    dma = pltpu.SemaphoreType.DMA
    return pl.pallas_call(
        functools.partial(fold_body, dims, colors, pieces, len(bufs)),
        out_shape=jax.ShapeDtypeStruct((lines, LANES), jnp.float32),
        in_specs=[pl.BlockSpec(memory_space=pl.ANY)],
        out_specs=pl.BlockSpec(memory_space=pl.ANY),
        scratch_shapes=[
            pltpu.VMEM((*grid, lines, LANES), jnp.float32),
            *bufs,
            dma((len(bufs), pieces)),
            dma((len(bufs), pieces)),
            dma,
        ],
        name=name,
        compiler_params=pltpu.CompilerParams(
            collective_id=collective_id, has_side_effects=True, vmem_limit_bytes=VMEM_MAX
        ),
    )(part_lines.reshape(*grid, lines, LANES))


def solution(mesh):
    size_z = mesh.shape["gz"]
    size_y = mesh.shape["gy"]
    size_x = mesh.shape["gx"]
    n_dev = size_z * size_y * size_x

    def device_step(nz_vals, idx_i, idx_j, idx_k, fac_a, fac_b, fac_c):
        own_a, own_b, own_c = fac_a.shape[0], fac_b.shape[0], fac_c.shape[0]
        rows_a = lines_of(own_a) * (n_dev // size_x)
        rows_b = lines_of(own_b) * (n_dev // size_y)
        rows_c = lines_of(own_c) * (n_dev // size_z)
        old_a, old_b, old_c = fac_a.T, fac_b.T, fac_c.T

        sizes = (("gx", size_x), ("gz", size_z), ("gy", size_y))
        spec_a = ("gz", size_z, "gy", size_y)
        spec_b = ("gz", size_z, "gx", size_x)
        spec_c = ("gy", size_y, "gx", size_x)
        pack_b, pack_c, grams = prep(old_b, old_c)
        buf_c, buf_b = expand_slabs("gather_bc", 0, (spec_c, spec_b), (pack_c, pack_b))
        grams = sum_all("sum_bc", 1, sizes, grams)
        gram_b, gram_c = grams[:RANK], grams[RANK:]

        at_a = place_rows(idx_i, own_a)
        at_b = place_rows(idx_j, own_b)
        at_c = place_rows(idx_k, own_c)
        used = jnp.max(jnp.where(nz_vals != 0, jnp.arange(nz_vals.shape[0], dtype=jnp.int32) + 1, 1))
        nblk = ((used + (BLOCK - 1)) // BLOCK).reshape(1)

        plan_a = plan_mode(nblk, nz_vals, at_a, at_b, at_c, rows_a)
        part_a = mttkrp("mttkrp_a", plan_a, buf_b, buf_c, rows_a)
        inv, mu = invert("invert_a", gram_b, gram_c)
        fresh, gram = solve("solve_a", fold_slab("fold_a", 7, "a", part_a), old_a, inv, mu)
        out_a, _, gram_a, pack_a = scale("scale_a", fresh, sum_all("sum_a", 2, sizes, gram), own_a * n_dev, True)
        (buf_a,) = expand_slabs("gather_a", 3, (spec_a,), (pack_a,))

        plan_b = plan_mode(nblk, nz_vals, at_b, at_a, at_c, rows_b)
        part_b = mttkrp("mttkrp_b", plan_b, buf_a, buf_c, rows_b)
        inv, mu = invert("invert_b", gram_a, gram_c)
        fresh, gram = solve("solve_b", fold_slab("fold_b", 8, "b", part_b), old_b, inv, mu)
        out_b, _, gram_nb, pack_nb = scale("scale_b", fresh, sum_all("sum_b", 4, sizes, gram), own_b * n_dev, True)
        (buf_nb,) = expand_slabs("gather_b", 5, (spec_b,), (pack_nb,))

        plan_c = plan_mode(nblk, nz_vals, at_c, at_a, at_b, rows_c)
        part_c = mttkrp("mttkrp_c", plan_c, buf_a, buf_nb, rows_c)
        inv, mu = invert("invert_c", gram_a, gram_nb)
        fresh, gram = solve("solve_c", fold_slab("fold_c", 9, "c", part_c), old_c, inv, mu)
        out_c, lambdas, _ = scale("scale_c", fresh, sum_all("sum_c", 6, sizes, gram), own_c * n_dev, False)
        return out_a.T, out_b.T, out_c.T, lambdas.reshape(RANK)

    part_nz = P(("gz", "gy", "gx"))
    part_a = P(("gx", "gz", "gy"), None)
    part_b = P(("gy", "gz", "gx"), None)
    part_c = P(("gz", "gy", "gx"), None)
    return jax.shard_map(
        device_step,
        mesh=mesh,
        in_specs=(part_nz, part_nz, part_nz, part_nz, part_a, part_b, part_c),
        out_specs=(part_a, part_b, part_c, P()),
        check_vma=False,
    )
```
